32 devices in a mesh: seq: 8 (over y, x, core), batch: 4 (over z).
Axes of the slice: x: 2, y: 2, z: 4, core: 2. Of those that a mesh axis runs over, the one named last changes fastest.
Arguments:
- queries: bfloat16 [4096, 4096], P(('batch', 'seq')), parts along dimension 0, may hold values from -6 to 6
- key_vectors: bfloat16 [4096, 4096], P(('batch', 'seq')), parts along dimension 0, may hold values from -6 to 6
- value_vectors: bfloat16 [4096, 4096], P(('batch', 'seq')), parts along dimension 0, may hold values from -6 to 6
- residual_in: bfloat16 [4096, 4096], P(('batch', 'seq')), parts along dimension 0, may hold values from -6 to 6
- input_logit: float32 [8, 4096], P(None, ('batch', 'seq')), parts along dimension 1, may hold values from -8 to 300
- forget_logit: float32 [8, 4096], P(None, ('batch', 'seq')), parts along dimension 1, may hold values from -3 to 13
- mix_gain: float32 [4096], replicated, may hold values from 0.1 to 1.9
- ffn_gain: float32 [4096], replicated, may hold values from 0.1 to 1.9
- expert_gate: bfloat16 [8, 4096, 704], P('seq'), may hold values from -0.09375 to 0.09375
- expert_up: bfloat16 [8, 4096, 704], P('seq'), may hold values from -0.09375 to 0.09375
- expert_down: bfloat16 [8, 704, 4096], P('seq'), may hold values from -0.21875 to 0.21875
- routes: int32 [4096, 2], P(('batch', 'seq')), parts along dimension 0, may hold values from 0 to 7, all different within a row; in each aligned block of 128 rows (0 to 127, 128 to 255, ...) at most 64 rows name the same one
- route_weight: float32 [4096, 2], P(('batch', 'seq')), parts along dimension 0, may hold values from 0.2 to 1
Outputs:
- block_out: bfloat16 [4096, 4096], P(('batch', 'seq')), parts along dimension 0
The draws below stay inside these ranges and needn't reach their ends.
There are 4 independent parts, one for each index of `batch`. The reference program is written for one: setup_inputs(seed, part) draws one part's arguments, and reference() takes and returns one part's arrays. A program takes and returns all parts, laid end to end along the dimension named above; an argument that names none is the same for every part. Nothing has to cross between parts.
Inputs may be any that keep to these rules, and one draw needn't show every extreme that they name: `routes`: each row names two different experts. Within the rows of one device no expert is named by more than 64 rows, and in some device one expert is named by exactly 64 rows.
All inputs are finite; a program needn't handle non-finite values.
Results may differ from the reference program's by a relative error of at most 0.0081.
Values may be sent and summed in bfloat16 or wider, within the bound.
No kernel may reach another device: no remote copies, remote signals or barrier semaphores. Data moves between devices by JAX's collectives and lax.ppermute only.
A program may use at most 128 MiB of HBM per device.

```python
import math
import jax
import jax.numpy as jnp
import numpy as np
from jax import lax

MIXER_HEADS = 8
DH = 512
D = 4096
FF = 704
TOK_DEV = 128
SEQUENCE_LENGTH = 1024
EXPERTS = 8
CAP = 64


def draw_forget_logit(key, part):
    random_child_keys = jax.random.split(jax.random.fold_in(key, 11), 6)
    chooser = jax.random.uniform(random_child_keys[0], (MIXER_HEADS, 1))
    quick_head = chooser < 0.5
    horizon = TOK_DEV * jax.random.uniform(random_child_keys[1], (MIXER_HEADS, 1), minval=0.15, maxval=0.25)
    slow_rate = jnp.log(1.0 / 0.7) / SEQUENCE_LENGTH * jnp.ones((MIXER_HEADS, 1), jnp.float32)
    base_rate = jnp.where(quick_head, 1.0 / horizon, slow_rate)
    blocks = SEQUENCE_LENGTH // TOK_DEV
    device_factor = jnp.exp(jax.random.uniform(random_child_keys[2], (MIXER_HEADS, blocks), minval=-0.7, maxval=0.7))
    device_factor = jnp.repeat(device_factor, TOK_DEV, axis=1)
    roughness = jax.random.uniform(random_child_keys[3], (MIXER_HEADS, SEQUENCE_LENGTH), minval=0.5, maxval=1.5)
    forget_decay_speed = base_rate * device_factor * roughness
    spike_locations = jax.random.randint(random_child_keys[4], (3,), 0, SEQUENCE_LENGTH)
    spike_present = jnp.any(jnp.arange(SEQUENCE_LENGTH)[None, :] == spike_locations[:, None], axis=0)[None, :]
    spike_frequency = jax.random.uniform(random_child_keys[5], (MIXER_HEADS, SEQUENCE_LENGTH), minval=0.22, maxval=0.69)
    forget_decay_speed = jnp.where(spike_present, spike_frequency, forget_decay_speed)
    return jnp.log(1.0 / jnp.expm1(forget_decay_speed)).astype(jnp.float32)


def draw_input_logit(key, part):
    random_child_keys = jax.random.split(jax.random.fold_in(key, 23), 5)
    drawn = jax.random.normal(random_child_keys[4], (MIXER_HEADS, SEQUENCE_LENGTH)) * 1.5 - 1.0
    return jnp.clip(drawn, -8.0, 8.0).astype(jnp.float32)


def block_levels(rng, dims, shards, least, largest):
    def one(dim, blocks):
        draws = jax.random.uniform(jax.random.fold_in(jax.random.fold_in(rng, 6), dim), (blocks,), jnp.float32, least / len(shards), largest / len(shards))
        return jnp.repeat(jnp.exp(draws), dims[dim] // blocks).reshape((-1,) + (1,) * (len(dims) - dim - 1))

    gain = one(*shards[0])
    for cut in shards[1:]:
        gain = gain * one(*cut)
    return gain


def shared_out(key, own, number, rows, number_of, top, reach, lean):
    sequence = jax.random.permutation(key, number_of)
    crowded, common = portions_of(number_of, rows * top, reach, lean, True), portions_of(number_of, rows * top, reach, lean, False)
    places = jnp.arange(number_of)

    def named(sizes, turn):
        used = int((sizes > 0).sum())
        fixed = max(1, used // 4)
        shifted = fixed + (places - fixed + turn * (used - fixed)) % max(1, number_of - fixed)
        return jnp.zeros((number_of,), jnp.int32).at[sequence[jnp.where(places < fixed, places, shifted)]].set(jnp.asarray(sizes, jnp.int32))

    sizes = jnp.where(number % 4 == 0, named(crowded, number // 4), named(common, number - number // 4 - 1))
    mixed = jax.random.permutation(jax.random.fold_in(own, 3), number_of)
    donor, receiver = mixed[0:number_of // 2 * 2:2], mixed[1:number_of // 2 * 2:2]
    slack = jnp.minimum(sizes[donor] - 1, reach - sizes[receiver]) // 2
    slack = jnp.where((donor == sequence[0]) | (receiver == sequence[0]) | (sizes[receiver] == 0), 0, jnp.maximum(slack, 0))
    shifted = jax.random.randint(jax.random.fold_in(own, 4), (number_of // 2,), 0, 1 << 20) % (slack + 1)
    sizes = sizes.at[donor].add(-shifted).at[receiver].add(shifted)
    members = jnp.searchsorted(jnp.cumsum(sizes), jnp.arange(rows * top), side="right").astype(jnp.int32)
    grid = members.reshape(top, rows).T
    grid = grid[jax.random.permutation(jax.random.fold_in(own, 1), rows)]
    turn = jax.random.randint(jax.random.fold_in(own, 2), (rows, 1), 0, top)
    return jnp.take_along_axis(grid, (jnp.arange(top)[None, :] + turn) % top, axis=1)


def portions_of(amount, total, limit, skew, full):
    weights = [(1 << 20) // math.isqrt(standing ** skew) + 1 for standing in range(1, amount + 1)]
    largest = limit if full else min(limit, max(-(-total // amount), total * weights[0] // sum(weights)))
    least = 1 if total - largest >= amount - 1 else 0
    given, surplus = [largest] + [least] * (amount - 1), total - largest - least * (amount - 1)
    while surplus > 0:
        free = [i for i in range(1, amount) if given[i] < largest] or [i for i in range(1, amount) if given[i] < limit]
        whole, remaining = sum([weights[i] for i in free]), surplus
        for i in free:
            more = min(limit - given[i], max(1, remaining * weights[i] // whole), surplus)
            given[i] = given[i] + more
            surplus = surplus - more
    return np.array(given)


def scatter_about(own_key, extent, spread, bound, cuts=(), kind=jnp.bfloat16):
    entries = spread * jax.random.normal(own_key, extent, jnp.float32)
    if cuts:
        entries = entries * block_levels(own_key, extent, cuts, -0.22, 0.18)
    return jnp.clip(entries, -bound, bound).astype(kind)


def setup_inputs(seed: int = 0, part: int = 0) -> dict:
    seeds = jax.random.split(jax.random.key(seed), 14)
    own_keys = jax.random.split(jax.random.fold_in(seeds[13], part), 14)
    queries = scatter_about(own_keys[0], (SEQUENCE_LENGTH, D), 1.0, 6.0, ((0, 8),))
    key_vectors = scatter_about(own_keys[1], (SEQUENCE_LENGTH, D), 1.0, 6.0, ((0, 8),))
    value_vectors = scatter_about(own_keys[2], (SEQUENCE_LENGTH, D), 1.0, 6.0, ((0, 8),))
    residual_in = scatter_about(own_keys[3], (SEQUENCE_LENGTH, D), 1.0, 6.0, ((0, 8),))
    input_logit = draw_input_logit(jax.random.fold_in(jax.random.fold_in(seeds[13], part), 71), part)
    forget_logit = draw_forget_logit(jax.random.fold_in(jax.random.fold_in(seeds[13], part), 71), part)
    mix_gain = jnp.clip(1.0 + 0.18 * jax.random.normal(seeds[6], (D,), jnp.float32), 0.1, 1.9)
    ffn_gain = jnp.clip(1.0 + 0.18 * jax.random.normal(seeds[7], (D,), jnp.float32), 0.1, 1.9)
    expert_gate = scatter_about(seeds[8], (EXPERTS, D, FF), D ** -0.5, 0.09375, ((0, 8),))
    expert_up = scatter_about(seeds[9], (EXPERTS, D, FF), D ** -0.5, 0.09375, ((0, 8),))
    expert_down = scatter_about(seeds[10], (EXPERTS, FF, D), FF ** -0.5, 0.21875, ((0, 8),))
    routes_keys = jax.random.split(jax.random.fold_in(own_keys[11], 1), SEQUENCE_LENGTH // TOK_DEV)
    routes_turns = jax.random.permutation(jax.random.fold_in(own_keys[11], 3), SEQUENCE_LENGTH // TOK_DEV)
    routes = jax.vmap(lambda own, number: shared_out(jax.random.fold_in(own_keys[11], 2), own, number, TOK_DEV, EXPERTS, 2, CAP, 2))(routes_keys, routes_turns).reshape((SEQUENCE_LENGTH, 2))
    route_weight = jnp.clip(0.2 + 0.8 * jax.random.uniform(own_keys[12], (SEQUENCE_LENGTH, 2), jnp.float32) ** block_levels(own_keys[12], (SEQUENCE_LENGTH, 2), ((0, 8),), -0.2, 0.2), 0.2, 1.0)
    return dict(queries=queries, key_vectors=key_vectors, value_vectors=value_vectors, residual_in=residual_in, input_logit=input_logit, forget_logit=forget_logit, mix_gain=mix_gain, ffn_gain=ffn_gain, expert_gate=expert_gate, expert_up=expert_up, expert_down=expert_down, routes=routes, route_weight=route_weight)


NEG_FILL = -1e+30
EPSILON = 1e-06

def join_states(earlier, later):
    total_early, state_early, normv_early, peak_early = earlier
    total_late, state_late, normv_late, peak_late = later
    carried = total_late + peak_early
    peak_new = jnp.maximum(carried, peak_late)
    scale_early = jnp.exp(carried - peak_new)
    scale_late = jnp.exp(peak_late - peak_new)
    state_new = scale_early[..., None] * state_early + scale_late[..., None] * state_late
    normv_new = scale_early * normv_early + scale_late * normv_late
    return (total_early + total_late, state_new, normv_new, peak_new)

def block_summary(keys_three, values_three, log_forget, input_gate):
    cumul_log = jnp.cumsum(log_forget, axis=1)
    tail_log = cumul_log[:, -1:] - cumul_log + input_gate
    peak_log = lax.optimization_barrier(jnp.max(tail_log, axis=1))
    weight = jnp.exp(tail_log - peak_log[:, None])
    weighted = keys_three.astype(jnp.float32) * jnp.transpose(weight)[:, :, None]
    rounded = lax.optimization_barrier(weighted.astype(jnp.bfloat16))
    state_mat = jnp.einsum('thd,the->hde', rounded.astype(jnp.float32), values_three.astype(jnp.float32))
    norm_vec = lax.optimization_barrier(jnp.sum(weighted, axis=0))
    total_log = jnp.broadcast_to(cumul_log[:, -1:], norm_vec.shape)
    peak_full = jnp.broadcast_to(peak_log[:, None], norm_vec.shape)
    return (total_log, state_mat, norm_vec, peak_full)

def block_output(queries_three, keys_three, values_three, log_forget, input_gate, carry_in):
    length_block = queries_three.shape[0]
    inverse_root = 1.0 / math.sqrt(queries_three.shape[2])
    cumul_log = jnp.cumsum(log_forget, axis=1)
    log_weight = cumul_log[:, :, None] - cumul_log[:, None, :] + input_gate[:, None, :]
    causal = jnp.arange(length_block)[:, None] >= jnp.arange(length_block)[None, :]
    log_weight = jnp.where(causal[None], log_weight, NEG_FILL)
    carry_total, carry_state, carry_norm, carry_peak = carry_in
    carried = cumul_log + carry_peak[:, 0:1]
    peak_log = jnp.maximum(lax.optimization_barrier(jnp.max(log_weight, axis=2)), carried)
    decay_mat = jnp.exp(log_weight - peak_log[:, :, None])
    query_float = queries_three.astype(jnp.float32)
    scores = jnp.einsum('thd,shd->hts', query_float, keys_three.astype(jnp.float32)) * inverse_root
    coef = decay_mat * scores
    denom_sum = lax.optimization_barrier(jnp.sum(coef, axis=2))
    coef_round = lax.optimization_barrier(coef.astype(jnp.bfloat16))
    numer_sum = jnp.einsum('hts,she->the', coef_round.astype(jnp.float32), values_three.astype(jnp.float32))
    carry_reach = jnp.exp(carried - peak_log) * inverse_root
    from_state = jnp.einsum('thd,hde->the', query_float, carry_state, precision=lax.Precision.HIGHEST)
    from_norm = jnp.einsum('thd,hd->ht', query_float, carry_norm, precision=lax.Precision.HIGHEST)
    numer_sum = numer_sum + jnp.transpose(carry_reach)[:, :, None] * from_state
    denom_sum = denom_sum + carry_reach * from_norm
    floor_sum = jnp.maximum(jnp.abs(denom_sum), 1.0)
    return numer_sum / jnp.transpose(floor_sum)[:, :, None]

def reference(queries, key_vectors, value_vectors, residual_in, input_logit, forget_logit, mix_gain, ffn_gain, expert_gate, expert_up, expert_down, routes, route_weight):
    log_forget = jax.nn.log_sigmoid(forget_logit)
    blocks = SEQUENCE_LENGTH // TOK_DEV

    def split_rows(array):
        return array.reshape(blocks, TOK_DEV, MIXER_HEADS, DH)

    def split_gates(array):
        return jnp.transpose(array.reshape(MIXER_HEADS, blocks, TOK_DEV), (1, 0, 2))
    initial = (jnp.zeros((MIXER_HEADS, DH), jnp.float32), jnp.zeros((MIXER_HEADS, DH, DH), jnp.float32), jnp.zeros((MIXER_HEADS, DH), jnp.float32), jnp.full((MIXER_HEADS, DH), NEG_FILL, jnp.float32))

    def advance(carry_in, pieces):
        query_block, key_block, value_block, forget_block, input_block = pieces
        result = block_output(query_block, key_block, value_block, forget_block, input_block, carry_in)
        carry_out = join_states(carry_in, block_summary(key_block, value_block, forget_block, input_block))
        return (carry_out, result)
    unused, mixer_out = lax.scan(advance, initial, (split_rows(queries), split_rows(key_vectors), split_rows(value_vectors), split_gates(log_forget), split_gates(input_logit)))
    mixer_out = mixer_out.reshape(SEQUENCE_LENGTH, D)
    mixer_square = lax.optimization_barrier(jnp.mean(mixer_out * mixer_out, axis=1, keepdims=True))
    updated = (residual_in.astype(jnp.float32) + mixer_out * lax.rsqrt(mixer_square + EPSILON) * mix_gain).astype(jnp.bfloat16)
    updated_float = updated.astype(jnp.float32)
    updated_square = lax.optimization_barrier(jnp.mean(updated_float * updated_float, axis=1, keepdims=True))
    normed = (updated_float * lax.rsqrt(updated_square + EPSILON) * ffn_gain).astype(jnp.bfloat16)
    flat_routes = routes.reshape(blocks, 2 * TOK_DEV)
    matches = (flat_routes[:, :, None] == jnp.arange(EXPERTS, dtype=jnp.int32)[None, None, :]).astype(jnp.int32)
    before = jnp.cumsum(matches, axis=1) - matches
    position = lax.optimization_barrier(jnp.sum(before * matches, axis=2))
    source_index = jnp.arange(blocks, dtype=jnp.int32)[:, None]
    slot_index = (flat_routes * (blocks * CAP) + source_index * CAP + position).reshape(SEQUENCE_LENGTH, 2).astype(jnp.int32)
    buffer_rows = jnp.zeros((EXPERTS * blocks * CAP, D), jnp.bfloat16)
    buffer_rows = buffer_rows.at[slot_index[:, 0]].set(normed).at[slot_index[:, 1]].set(normed)

    def run_expert(pieces):
        row_block, gate_weight, up_weight, down_weight = pieces
        gate_val = jnp.dot(row_block, gate_weight, preferred_element_type=jnp.float32)
        up_val = jnp.dot(row_block, up_weight, preferred_element_type=jnp.float32)
        hidden = (jax.nn.silu(gate_val) * up_val).astype(jnp.bfloat16)
        return jnp.dot(hidden, down_weight, preferred_element_type=jnp.float32).astype(jnp.bfloat16)
    outputs = lax.map(run_expert, (buffer_rows.reshape(EXPERTS, blocks * CAP, D), expert_gate, expert_up, expert_down)).reshape(EXPERTS * blocks * CAP, D)
    first_out = outputs[slot_index[:, 0]].astype(jnp.float32)
    second_out = outputs[slot_index[:, 1]].astype(jnp.float32)
    expert_mix = route_weight[:, 0:1] * first_out + route_weight[:, 1:2] * second_out
    return (updated_float + expert_mix).astype(jnp.bfloat16)
```

```python
import functools
import math

import jax
import jax.numpy as jnp
from jax import lax
from jax.experimental import pallas as pl
from jax.experimental.pallas import tpu as pltpu
from jax.sharding import PartitionSpec as P

NEG_FILL = -1e30
EPSILON = 1e-06
GATE_ROWS = 8


def three_parts(value):
    high = value.astype(jnp.bfloat16)
    rest = value - high.astype(jnp.float32)
    middle = rest.astype(jnp.bfloat16)
    low = (rest - middle.astype(jnp.float32)).astype(jnp.bfloat16)
    return [high, middle, low]


def pack_kernel(query_ref, key_ref, value_ref, input_ref, forget_ref, out_ref, *, group):
    tokens, head_dim = query_ref.shape
    width = value_ref.shape[1]
    out_ref[0, :tokens, :head_dim] = query_ref[...]
    out_ref[0, :tokens, head_dim : 2 * head_dim] = key_ref[...]
    out_ref[0, :tokens, 2 * head_dim :] = value_ref[...]
    head = pl.program_id(0) // group
    gates = [input_ref[pl.ds(head, 1), :], forget_ref[pl.ds(head, 1), :]]
    column = 0
    for gate in gates:
        spread = jnp.broadcast_to(gate, (GATE_ROWS, tokens))
        for part in three_parts(spread):
            out_ref[0, tokens:, column : column + tokens] = part
            column += tokens
    left = 2 * head_dim + width - column
    out_ref[0, tokens:, column:] = jnp.zeros((GATE_ROWS, left), jnp.bfloat16)


def pack(queries, keys, values, input_logit, forget_logit, devices):
    tokens, model_width = queries.shape
    heads = input_logit.shape[0]
    head_dim = model_width // heads
    group = devices // heads
    width = model_width // devices
    full = 2 * head_dim + width
    gate_spec = pl.BlockSpec((heads, tokens), lambda i: (0, 0))
    return pl.pallas_call(
        functools.partial(pack_kernel, group=group),
        grid=(devices,),
        in_specs=[
            pl.BlockSpec((tokens, head_dim), lambda i: (0, i // group)),
            pl.BlockSpec((tokens, head_dim), lambda i: (0, i // group)),
            pl.BlockSpec((tokens, width), lambda i: (0, i)),
            gate_spec,
            gate_spec,
        ],
        out_specs=pl.BlockSpec((1, tokens + GATE_ROWS, full), lambda i: (i, 0, 0)),
        out_shape=jax.ShapeDtypeStruct((devices, tokens + GATE_ROWS, full), jnp.bfloat16),
        name="pack",
    )(queries, keys, values, input_logit, forget_logit)


def mix_kernel(packed_ref, gate_ref, out_ref, rows_ref, sems, *, head_dim):
    devices, tokens, width = out_ref.shape

    def load(block):
        return pltpu.make_async_copy(
            packed_ref.at[block, pl.ds(0, tokens), :],
            rows_ref.at[pl.ds(block * tokens, tokens), :],
            sems.at[block],
        )

    for block in range(devices):
        load(block).start()
    inverse_root = 1.0 / math.sqrt(head_dim)
    input_rows = []
    forget_rows = []
    for block in range(devices):
        parts = gate_ref[block].astype(jnp.float32)
        pieces = [parts[0:1, i * tokens : (i + 1) * tokens] for i in range(6)]
        input_rows.append(pieces[0] + pieces[1] + pieces[2])
        forget_rows.append(pieces[3] + pieces[4] + pieces[5])
    log_forget = jax.nn.log_sigmoid(jnp.concatenate(forget_rows, axis=0))
    upper = (
        lax.broadcasted_iota(jnp.int32, (tokens, tokens), 0)
        <= lax.broadcasted_iota(jnp.int32, (tokens, tokens), 1)
    ).astype(jnp.float32)
    cumul = jnp.dot(
        log_forget, upper, precision=lax.Precision.HIGHEST, preferred_element_type=jnp.float32
    )
    earlier = None
    for block in range(devices):
        seen = (block + 1) * tokens
        own = input_rows[block] - cumul[block : block + 1, :]
        row = own if earlier is None else jnp.concatenate([earlier, own], axis=1)
        earlier = row + cumul[block : block + 1, tokens - 1 : tokens]
        causal = lax.broadcasted_iota(jnp.int32, (tokens, seen), 1) <= (
            lax.broadcasted_iota(jnp.int32, (tokens, seen), 0) + block * tokens
        )
        log_weight = jnp.where(causal, jnp.broadcast_to(row, (tokens, seen)), NEG_FILL)
        peak = jnp.max(log_weight, axis=1, keepdims=True)
        load(block).wait()
        query = rows_ref[block * tokens : seen, :head_dim]
        scores = lax.dot_general(
            query,
            rows_ref[:seen, head_dim : 2 * head_dim],
            (((1,), (1,)), ((), ())),
            preferred_element_type=jnp.float32,
        )
        coef = jnp.exp(log_weight - peak) * (scores * inverse_root)
        denom = jnp.sum(coef, axis=1, keepdims=True)
        numer = jnp.dot(
            coef.astype(jnp.bfloat16),
            rows_ref[:seen, 2 * head_dim :],
            preferred_element_type=jnp.float32,
        )
        out_ref[block] = (numer / jnp.maximum(jnp.abs(denom), 1.0)).astype(jnp.bfloat16)


def mix(packed, tokens, head_dim):
    devices, padded, full = packed.shape
    width = full - 2 * head_dim
    return pl.pallas_call(
        functools.partial(mix_kernel, head_dim=head_dim),
        grid=(1,),
        in_specs=[
            pl.BlockSpec(memory_space=pl.ANY),
            pl.BlockSpec(
                (devices, GATE_ROWS, 6 * tokens), lambda i: (0, tokens // GATE_ROWS, 0)
            ),
        ],
        out_specs=pl.BlockSpec((devices, tokens, width), lambda i: (0, 0, 0)),
        out_shape=jax.ShapeDtypeStruct((devices, tokens, width), jnp.bfloat16),
        scratch_shapes=[
            pltpu.VMEM((devices * tokens, full), jnp.bfloat16),
            pltpu.SemaphoreType.DMA((devices,)),
        ],
        name="mix",
    )(packed, packed)


def norm_kernel(
    mixed_ref, residual_ref, mix_gain_ref, ffn_gain_ref, slot_ref, updated_ref, out_ref, normed_ref
):
    pieces, tokens, width = mixed_ref.shape
    model_width = pieces * width
    step = pl.program_id(0)

    @pl.when(step == 0)
    def _():
        square = jnp.zeros((tokens, 1), jnp.float32)
        for i in range(pieces):
            piece = mixed_ref[i].astype(jnp.float32)
            square = square + jnp.sum(piece * piece, axis=1, keepdims=True)
        scale = lax.rsqrt(square / model_width + EPSILON)
        square = jnp.zeros((tokens, 1), jnp.float32)
        for i in range(pieces):
            cols = pl.ds(i * width, width)
            piece = mixed_ref[i].astype(jnp.float32)
            updated = (
                residual_ref[:, cols].astype(jnp.float32) + piece * scale * mix_gain_ref[:, cols]
            ).astype(jnp.bfloat16)
            updated_ref[:, cols] = updated
            updated = updated.astype(jnp.float32)
            square = square + jnp.sum(updated * updated, axis=1, keepdims=True)
        scale = lax.rsqrt(square / model_width + EPSILON)
        for i in range(pieces):
            cols = pl.ds(i * width, width)
            updated = updated_ref[:, cols].astype(jnp.float32)
            normed_ref[i] = (updated * scale * ffn_gain_ref[:, cols]).astype(jnp.bfloat16)

    slots = out_ref.shape[0]
    place = lax.broadcasted_iota(jnp.int32, (slots, tokens), 0)
    chosen = (place == slot_ref[0:1, :]) | (place == slot_ref[1:2, :])
    pick = jnp.where(chosen, 1.0, 0.0).astype(jnp.bfloat16)
    out_ref[...] = jnp.dot(
        pick, normed_ref[step], preferred_element_type=jnp.float32
    ).astype(jnp.bfloat16)


def norm_and_spread(mixed, residual, mix_gain, ffn_gain, slot_rows, slots):
    pieces, tokens, width = mixed.shape
    model_width = pieces * width
    whole = pl.BlockSpec((tokens, model_width), lambda i: (0, 0))
    gain = pl.BlockSpec((1, model_width), lambda i: (0, 0))
    return pl.pallas_call(
        norm_kernel,
        grid=(pieces,),
        in_specs=[
            pl.BlockSpec((pieces, tokens, width), lambda i: (0, 0, 0)),
            whole,
            gain,
            gain,
            pl.BlockSpec((2, tokens), lambda i: (0, 0)),
        ],
        out_specs=[whole, pl.BlockSpec((slots, width), lambda i: (0, i))],
        out_shape=[
            jax.ShapeDtypeStruct((tokens, model_width), jnp.bfloat16),
            jax.ShapeDtypeStruct((slots, model_width), jnp.bfloat16),
        ],
        scratch_shapes=[pltpu.VMEM((pieces, tokens, width), jnp.bfloat16)],
        name="norm_spread",
    )(mixed, residual, mix_gain[None], ffn_gain[None], slot_rows)


def combine_kernel(back_ref, updated_ref, slot_ref, weight_ref, out_ref):
    tokens = updated_ref.shape[0]
    slots = back_ref.shape[0]
    place = lax.broadcasted_iota(jnp.int32, (tokens, slots), 1)
    back = back_ref[...]
    total = updated_ref[...].astype(jnp.float32)
    for k in range(2):
        pick = jnp.where(place == slot_ref[:, k : k + 1], 1.0, 0.0).astype(jnp.bfloat16)
        rows = jnp.dot(pick, back, preferred_element_type=jnp.float32)
        total = total + weight_ref[:, k : k + 1] * rows
    out_ref[...] = total.astype(jnp.bfloat16)


def combine(back, updated, slot_index, route_weight, pieces):
    slots, model_width = back.shape
    tokens = updated.shape[0]
    width = model_width // pieces
    pair = pl.BlockSpec((tokens, 2), lambda i: (0, 0))
    return pl.pallas_call(
        combine_kernel,
        grid=(pieces,),
        in_specs=[
            pl.BlockSpec((slots, width), lambda i: (0, i)),
            pl.BlockSpec((tokens, width), lambda i: (0, i)),
            pair,
            pair,
        ],
        out_specs=pl.BlockSpec((tokens, width), lambda i: (0, i)),
        out_shape=jax.ShapeDtypeStruct((tokens, model_width), jnp.bfloat16),
        name="combine",
    )(back, updated, slot_index, route_weight)


def shards(
    queries,
    key_vectors,
    value_vectors,
    residual_in,
    input_logit,
    forget_logit,
    mix_gain,
    ffn_gain,
    expert_gate,
    expert_up,
    expert_down,
    routes,
    route_weight,
):
    tokens, model_width = queries.shape
    head_count = input_logit.shape[0]
    head_dim = model_width // head_count
    devices = lax.axis_size("seq")

    def exchange(array):
        return lax.all_to_all(array, "seq", split_axis=0, concat_axis=0, tiled=True)

    capacity = 4 * tokens // devices
    slots = devices * capacity
    flat_routes = routes.reshape(-1)
    matches = (flat_routes[:, None] == jnp.arange(devices, dtype=jnp.int32)[None, :]).astype(
        jnp.int32
    )
    before = jnp.cumsum(matches, axis=0) - matches
    position = jnp.sum(before * matches, axis=1)
    slot_index = (flat_routes * capacity + position).reshape(tokens, 2)

    packed = exchange(
        pack(queries, key_vectors, value_vectors, input_logit, forget_logit, devices)
    )
    mixed = exchange(mix(packed, tokens, head_dim))
    updated, spread = norm_and_spread(
        mixed, residual_in, mix_gain, ffn_gain, jnp.transpose(slot_index), slots
    )
    block_in = exchange(spread.reshape(devices, capacity, model_width))
    row_block = block_in.reshape(-1, model_width)
    gate_val = jnp.dot(row_block, expert_gate[0], preferred_element_type=jnp.float32)
    up_val = jnp.dot(row_block, expert_up[0], preferred_element_type=jnp.float32)
    hidden = (jax.nn.silu(gate_val) * up_val).astype(jnp.bfloat16)
    result = jnp.dot(hidden, expert_down[0], preferred_element_type=jnp.float32).astype(
        jnp.bfloat16
    )
    inbound = exchange(result.reshape(block_in.shape))
    return combine(
        inbound.reshape(slots, model_width), updated, slot_index, route_weight, head_count
    )


def solution(mesh):
    return jax.shard_map(
        shards,
        mesh=mesh,
        in_specs=(
            P(("batch", "seq"), None),
            P(("batch", "seq"), None),
            P(("batch", "seq"), None),
            P(("batch", "seq"), None),
            P(None, ("batch", "seq")),
            P(None, ("batch", "seq")),
            P(),
            P(),
            P("seq", None, None),
            P("seq", None, None),
            P("seq", None, None),
            P(("batch", "seq"), None),
            P(("batch", "seq"), None),
        ),
        out_specs=P(("batch", "seq"), None),
        check_vma=False,
    )
```

```python
import functools
import math

import jax
import jax.numpy as jnp
from jax import lax
from jax.experimental import pallas as pl
from jax.experimental.pallas import tpu as pltpu
from jax.sharding import PartitionSpec as P

NEG_FILL = -1e30
EPSILON = 1e-06
GATE_ROWS = 8


def three_parts(value):
    high = value.astype(jnp.bfloat16)
    rest = value - high.astype(jnp.float32)
    middle = rest.astype(jnp.bfloat16)
    low = (rest - middle.astype(jnp.float32)).astype(jnp.bfloat16)
    return [high, middle, low]


def pack_kernel(query_ref, key_ref, value_ref, input_ref, forget_ref, out_ref, *, group):
    tokens, head_dim = query_ref.shape
    width = value_ref.shape[1]
    out_ref[0, :tokens, :head_dim] = query_ref[...]
    out_ref[0, :tokens, head_dim : 2 * head_dim] = key_ref[...]
    out_ref[0, :tokens, 2 * head_dim :] = value_ref[...]
    head = pl.program_id(0) // group
    gates = [input_ref[pl.ds(head, 1), :], forget_ref[pl.ds(head, 1), :]]
    column = 0
    for gate in gates:
        spread = jnp.broadcast_to(gate, (GATE_ROWS, tokens))
        for part in three_parts(spread):
            out_ref[0, tokens:, column : column + tokens] = part
            column += tokens
    left = 2 * head_dim + width - column
    out_ref[0, tokens:, column:] = jnp.zeros((GATE_ROWS, left), jnp.bfloat16)


def pack(queries, keys, values, input_logit, forget_logit, devices):
    tokens, model_width = queries.shape
    heads = input_logit.shape[0]
    head_dim = model_width // heads
    group = devices // heads
    width = model_width // devices
    full = 2 * head_dim + width
    gate_spec = pl.BlockSpec((heads, tokens), lambda i: (0, 0))
    return pl.pallas_call(
        functools.partial(pack_kernel, group=group),
        grid=(devices,),
        in_specs=[
            pl.BlockSpec((tokens, head_dim), lambda i: (0, i // group)),
            pl.BlockSpec((tokens, head_dim), lambda i: (0, i // group)),
            pl.BlockSpec((tokens, width), lambda i: (0, i)),
            gate_spec,
            gate_spec,
        ],
        out_specs=pl.BlockSpec((1, tokens + GATE_ROWS, full), lambda i: (i, 0, 0)),
        out_shape=jax.ShapeDtypeStruct((devices, tokens + GATE_ROWS, full), jnp.bfloat16),
        name="pack",
    )(queries, keys, values, input_logit, forget_logit)


def mix_kernel(packed_ref, gate_ref, out_ref, rows_ref, sems, *, head_dim):
    devices, tokens, width = out_ref.shape

    def load(block):
        return pltpu.make_async_copy(
            packed_ref.at[block, pl.ds(0, tokens), :],
            rows_ref.at[pl.ds(block * tokens, tokens), :],
            sems.at[block],
        )

    for block in range(devices):
        load(block).start()
    inverse_root = 1.0 / math.sqrt(head_dim)
    input_rows = []
    forget_rows = []
    for block in range(devices):
        parts = gate_ref[block].astype(jnp.float32)
        pieces = [parts[0:1, i * tokens : (i + 1) * tokens] for i in range(6)]
        input_rows.append(pieces[0] + pieces[1] + pieces[2])
        forget_rows.append(pieces[3] + pieces[4] + pieces[5])
    log_forget = jax.nn.log_sigmoid(jnp.concatenate(forget_rows, axis=0))
    upper = (
        lax.broadcasted_iota(jnp.int32, (tokens, tokens), 0)
        <= lax.broadcasted_iota(jnp.int32, (tokens, tokens), 1)
    ).astype(jnp.float32)
    cumul = jnp.dot(
        log_forget, upper, precision=lax.Precision.HIGHEST, preferred_element_type=jnp.float32
    )
    earlier = None
    for block in range(devices):
        seen = (block + 1) * tokens
        own = input_rows[block] - cumul[block : block + 1, :]
        row = own if earlier is None else jnp.concatenate([earlier, own], axis=1)
        earlier = row + cumul[block : block + 1, tokens - 1 : tokens]
        causal = lax.broadcasted_iota(jnp.int32, (tokens, seen), 1) <= (
            lax.broadcasted_iota(jnp.int32, (tokens, seen), 0) + block * tokens
        )
        log_weight = jnp.where(causal, jnp.broadcast_to(row, (tokens, seen)), NEG_FILL)
        peak = jnp.max(log_weight, axis=1, keepdims=True)
        load(block).wait()
        query = rows_ref[block * tokens : seen, :head_dim]
        scores = lax.dot_general(
            query,
            rows_ref[:seen, head_dim : 2 * head_dim],
            (((1,), (1,)), ((), ())),
            preferred_element_type=jnp.float32,
        )
        coef = jnp.exp(log_weight - peak) * (scores * inverse_root)
        denom = jnp.sum(coef, axis=1, keepdims=True)
        numer = jnp.dot(
            coef.astype(jnp.bfloat16),
            rows_ref[:seen, 2 * head_dim :],
            preferred_element_type=jnp.float32,
        )
        out_ref[block] = (numer / jnp.maximum(jnp.abs(denom), 1.0)).astype(jnp.bfloat16)


def mix(packed, tokens, head_dim):
    devices, padded, full = packed.shape
    width = full - 2 * head_dim
    return pl.pallas_call(
        functools.partial(mix_kernel, head_dim=head_dim),
        grid=(1,),
        in_specs=[
            pl.BlockSpec(memory_space=pl.ANY),
            pl.BlockSpec(
                (devices, GATE_ROWS, 6 * tokens), lambda i: (0, tokens // GATE_ROWS, 0)
            ),
        ],
        out_specs=pl.BlockSpec((devices, tokens, width), lambda i: (0, 0, 0)),
        out_shape=jax.ShapeDtypeStruct((devices, tokens, width), jnp.bfloat16),
        scratch_shapes=[
            pltpu.VMEM((devices * tokens, full), jnp.bfloat16),
            pltpu.SemaphoreType.DMA((devices,)),
        ],
        name="mix",
    )(packed, packed)


def norm_kernel(
    mixed_ref, residual_ref, mix_gain_ref, ffn_gain_ref, slot_ref, updated_ref, *rest
):
    *out_refs, normed_ref = rest
    pieces, tokens, width = mixed_ref.shape
    model_width = pieces * width
    step = pl.program_id(0)

    @pl.when(step == 0)
    def _():
        square = jnp.zeros((tokens, 1), jnp.float32)
        for i in range(pieces):
            piece = mixed_ref[i].astype(jnp.float32)
            square = square + jnp.sum(piece * piece, axis=1, keepdims=True)
        scale = lax.rsqrt(square / model_width + EPSILON)
        square = jnp.zeros((tokens, 1), jnp.float32)
        for i in range(pieces):
            cols = pl.ds(i * width, width)
            piece = mixed_ref[i].astype(jnp.float32)
            updated = (
                residual_ref[:, cols].astype(jnp.float32) + piece * scale * mix_gain_ref[:, cols]
            ).astype(jnp.bfloat16)
            updated_ref[:, cols] = updated
            updated = updated.astype(jnp.float32)
            square = square + jnp.sum(updated * updated, axis=1, keepdims=True)
        scale = lax.rsqrt(square / model_width + EPSILON)
        for i in range(pieces):
            cols = pl.ds(i * width, width)
            updated = updated_ref[:, cols].astype(jnp.float32)
            normed_ref[i] = (updated * scale * ffn_gain_ref[:, cols]).astype(jnp.bfloat16)

    for i, out_ref in enumerate(out_refs):
        rows = out_ref.shape[0]
        place = lax.broadcasted_iota(jnp.int32, (rows, tokens), 0) + i * rows
        chosen = (place == slot_ref[0:1, :]) | (place == slot_ref[1:2, :])
        pick = jnp.where(chosen, 1.0, 0.0).astype(jnp.bfloat16)
        out_ref[...] = jnp.dot(
            pick, normed_ref[step], preferred_element_type=jnp.float32
        ).astype(jnp.bfloat16)


def norm_and_spread(mixed, residual, mix_gain, ffn_gain, slot_rows, rows, chunks):
    pieces, tokens, width = mixed.shape
    model_width = pieces * width
    whole = pl.BlockSpec((tokens, model_width), lambda i: (0, 0))
    gain = pl.BlockSpec((1, model_width), lambda i: (0, 0))
    return pl.pallas_call(
        norm_kernel,
        grid=(pieces,),
        in_specs=[
            pl.BlockSpec((pieces, tokens, width), lambda i: (0, 0, 0)),
            whole,
            gain,
            gain,
            pl.BlockSpec((2, tokens), lambda i: (0, 0)),
        ],
        out_specs=[whole] + [pl.BlockSpec((rows, width), lambda i: (0, i))] * chunks,
        out_shape=[
            jax.ShapeDtypeStruct((tokens, model_width), jnp.bfloat16),
        ]
        + [jax.ShapeDtypeStruct((rows, model_width), jnp.bfloat16)] * chunks,
        scratch_shapes=[pltpu.VMEM((pieces, tokens, width), jnp.bfloat16)],
        name="norm_spread",
    )(mixed, residual, mix_gain[None], ffn_gain[None], slot_rows)


def combine_kernel(*refs):
    *back_refs, updated_ref, slot_ref, weight_ref, out_ref = refs
    tokens = updated_ref.shape[0]
    rows = back_refs[0].shape[0]
    place = lax.broadcasted_iota(jnp.int32, (tokens, rows), 1)
    total = updated_ref[...].astype(jnp.float32)
    for k in range(2):
        chosen = jnp.zeros((tokens, updated_ref.shape[1]), jnp.float32)
        for i, back_ref in enumerate(back_refs):
            match = place + i * rows == slot_ref[:, k : k + 1]
            pick = jnp.where(match, 1.0, 0.0).astype(jnp.bfloat16)
            chosen += jnp.dot(pick, back_ref[...], preferred_element_type=jnp.float32)
        total = total + weight_ref[:, k : k + 1] * chosen
    out_ref[...] = total.astype(jnp.bfloat16)


def combine(backs, updated, slot_index, route_weight, pieces):
    rows, model_width = backs[0].shape
    tokens = updated.shape[0]
    width = model_width // pieces
    pair = pl.BlockSpec((tokens, 2), lambda i: (0, 0))
    column = pl.BlockSpec((tokens, width), lambda i: (0, i))
    return pl.pallas_call(
        combine_kernel,
        grid=(pieces,),
        in_specs=[pl.BlockSpec((rows, width), lambda i: (0, i))] * len(backs)
        + [column, pair, pair],
        out_specs=column,
        out_shape=jax.ShapeDtypeStruct((tokens, model_width), jnp.bfloat16),
        name="combine",
    )(*backs, updated, slot_index, route_weight)


def shards(
    queries,
    key_vectors,
    value_vectors,
    residual_in,
    input_logit,
    forget_logit,
    mix_gain,
    ffn_gain,
    expert_gate,
    expert_up,
    expert_down,
    routes,
    route_weight,
):
    tokens, model_width = queries.shape
    head_count = input_logit.shape[0]
    head_dim = model_width // head_count
    devices = lax.axis_size("seq")

    def exchange(array):
        return lax.all_to_all(array, "seq", split_axis=0, concat_axis=0, tiled=True)

    capacity = 4 * tokens // devices
    chunks = 2
    part = capacity // chunks
    rows = devices * part
    flat_routes = routes.reshape(-1)
    matches = (flat_routes[:, None] == jnp.arange(devices, dtype=jnp.int32)[None, :]).astype(
        jnp.int32
    )
    before = jnp.cumsum(matches, axis=0) - matches
    position = jnp.sum(before * matches, axis=1)
    slot_index = (
        (position // part) * rows + flat_routes * part + position % part
    ).reshape(tokens, 2)

    packed = exchange(
        pack(queries, key_vectors, value_vectors, input_logit, forget_logit, devices)
    )
    mixed = exchange(mix(packed, tokens, head_dim))
    updated, *spread = norm_and_spread(
        mixed, residual_in, mix_gain, ffn_gain, jnp.transpose(slot_index), rows, chunks
    )
    results = []
    arrived = [exchange(one.reshape(devices, part, model_width)) for one in spread]
    for block_in in arrived:
        row_block = block_in.reshape(-1, model_width)
        gate_val = jnp.dot(row_block, expert_gate[0], preferred_element_type=jnp.float32)
        up_val = jnp.dot(row_block, expert_up[0], preferred_element_type=jnp.float32)
        hidden = (jax.nn.silu(gate_val) * up_val).astype(jnp.bfloat16)
        result = jnp.dot(hidden, expert_down[0], preferred_element_type=jnp.float32).astype(
            jnp.bfloat16
        )
        results.append(exchange(result.reshape(block_in.shape)).reshape(rows, model_width))
    return combine(results, updated, slot_index, route_weight, head_count)


def solution(mesh):
    return jax.shard_map(
        shards,
        mesh=mesh,
        in_specs=(
            P(("batch", "seq"), None),
            P(("batch", "seq"), None),
            P(("batch", "seq"), None),
            P(("batch", "seq"), None),
            P(None, ("batch", "seq")),
            P(None, ("batch", "seq")),
            P(),
            P(),
            P("seq", None, None),
            P("seq", None, None),
            P("seq", None, None),
            P(("batch", "seq"), None),
            P(("batch", "seq"), None),
        ),
        out_specs=P(("batch", "seq"), None),
        check_vma=False,
    )
```

```python
import functools
import math

import jax
import jax.numpy as jnp
from jax import lax
from jax.experimental import pallas as pl
from jax.experimental.pallas import tpu as pltpu
from jax.sharding import PartitionSpec as P

NEG_FILL = -1e30
EPSILON = 1e-06
GATE_ROWS = 8


def three_parts(value):
    high = value.astype(jnp.bfloat16)
    rest = value - high.astype(jnp.float32)
    middle = rest.astype(jnp.bfloat16)
    low = (rest - middle.astype(jnp.float32)).astype(jnp.bfloat16)
    return [high, middle, low]


def pack_kernel(query_ref, key_ref, value_ref, input_ref, forget_ref, out_ref, *, group):
    tokens, head_dim = query_ref.shape
    width = value_ref.shape[1]
    out_ref[0, :tokens, :head_dim] = query_ref[...]
    out_ref[0, :tokens, head_dim : 2 * head_dim] = key_ref[...]
    out_ref[0, :tokens, 2 * head_dim :] = value_ref[...]
    head = pl.program_id(0) // group
    gates = [input_ref[pl.ds(head, 1), :], forget_ref[pl.ds(head, 1), :]]
    column = 0
    for gate in gates:
        spread = jnp.broadcast_to(gate, (GATE_ROWS, tokens))
        for part in three_parts(spread):
            out_ref[0, tokens:, column : column + tokens] = part
            column += tokens
    left = 2 * head_dim + width - column
    out_ref[0, tokens:, column:] = jnp.zeros((GATE_ROWS, left), jnp.bfloat16)


def pack(queries, keys, values, input_logit, forget_logit, devices):
    tokens, model_width = queries.shape
    heads = input_logit.shape[0]
    head_dim = model_width // heads
    group = devices // heads
    width = model_width // devices
    full = 2 * head_dim + width
    gate_spec = pl.BlockSpec((heads, tokens), lambda i: (0, 0))
    return pl.pallas_call(
        functools.partial(pack_kernel, group=group),
        grid=(devices,),
        in_specs=[
            pl.BlockSpec((tokens, head_dim), lambda i: (0, i // group)),
            pl.BlockSpec((tokens, head_dim), lambda i: (0, i // group)),
            pl.BlockSpec((tokens, width), lambda i: (0, i)),
            gate_spec,
            gate_spec,
        ],
        out_specs=pl.BlockSpec((1, tokens + GATE_ROWS, full), lambda i: (i, 0, 0)),
        out_shape=jax.ShapeDtypeStruct((devices, tokens + GATE_ROWS, full), jnp.bfloat16),
        name="pack",
    )(queries, keys, values, input_logit, forget_logit)


def mix_kernel(packed_ref, gate_ref, out_ref, rows_ref, sems, *, head_dim):
    devices, tokens, width = out_ref.shape

    def load(block):
        return pltpu.make_async_copy(
            packed_ref.at[block, pl.ds(0, tokens), :],
            rows_ref.at[pl.ds(block * tokens, tokens), :],
            sems.at[block],
        )

    for block in range(devices):
        load(block).start()
    inverse_root = 1.0 / math.sqrt(head_dim)
    input_rows = []
    forget_rows = []
    for block in range(devices):
        parts = gate_ref[block].astype(jnp.float32)
        pieces = [parts[0:1, i * tokens : (i + 1) * tokens] for i in range(6)]
        input_rows.append(pieces[0] + pieces[1] + pieces[2])
        forget_rows.append(pieces[3] + pieces[4] + pieces[5])
    log_forget = jax.nn.log_sigmoid(jnp.concatenate(forget_rows, axis=0))
    upper = (
        lax.broadcasted_iota(jnp.int32, (tokens, tokens), 0)
        <= lax.broadcasted_iota(jnp.int32, (tokens, tokens), 1)
    ).astype(jnp.float32)
    cumul = jnp.dot(
        log_forget, upper, precision=lax.Precision.HIGHEST, preferred_element_type=jnp.float32
    )
    earlier = None
    for block in range(devices):
        seen = (block + 1) * tokens
        own = input_rows[block] - cumul[block : block + 1, :]
        row = own if earlier is None else jnp.concatenate([earlier, own], axis=1)
        earlier = row + cumul[block : block + 1, tokens - 1 : tokens]
        causal = lax.broadcasted_iota(jnp.int32, (tokens, seen), 1) <= (
            lax.broadcasted_iota(jnp.int32, (tokens, seen), 0) + block * tokens
        )
        log_weight = jnp.where(causal, jnp.broadcast_to(row, (tokens, seen)), NEG_FILL)
        peak = jnp.max(log_weight, axis=1, keepdims=True)
        load(block).wait()
        query = rows_ref[block * tokens : seen, :head_dim]
        scores = lax.dot_general(
            query,
            rows_ref[:seen, head_dim : 2 * head_dim],
            (((1,), (1,)), ((), ())),
            preferred_element_type=jnp.float32,
        )
        coef = jnp.exp(log_weight - peak) * (scores * inverse_root)
        denom = jnp.sum(coef, axis=1, keepdims=True)
        numer = jnp.dot(
            coef.astype(jnp.bfloat16),
            rows_ref[:seen, 2 * head_dim :],
            preferred_element_type=jnp.float32,
        )
        out_ref[block] = (numer / jnp.maximum(jnp.abs(denom), 1.0)).astype(jnp.bfloat16)


def mix(packed, tokens, head_dim):
    devices, padded, full = packed.shape
    width = full - 2 * head_dim
    return pl.pallas_call(
        functools.partial(mix_kernel, head_dim=head_dim),
        grid=(1,),
        in_specs=[
            pl.BlockSpec(memory_space=pl.ANY),
            pl.BlockSpec(
                (devices, GATE_ROWS, 6 * tokens), lambda i: (0, tokens // GATE_ROWS, 0)
            ),
        ],
        out_specs=pl.BlockSpec((devices, tokens, width), lambda i: (0, 0, 0)),
        out_shape=jax.ShapeDtypeStruct((devices, tokens, width), jnp.bfloat16),
        scratch_shapes=[
            pltpu.VMEM((devices * tokens, full), jnp.bfloat16),
            pltpu.SemaphoreType.DMA((devices,)),
        ],
        name="mix",
    )(packed, packed)


def norm_kernel(
    mixed_ref, residual_ref, mix_gain_ref, ffn_gain_ref, slot_ref, updated_ref, *rest
):
    *out_refs, normed_ref = rest
    pieces, tokens, width = mixed_ref.shape
    model_width = pieces * width
    step = pl.program_id(0)

    @pl.when(step == 0)
    def _():
        square = jnp.zeros((tokens, 1), jnp.float32)
        for i in range(pieces):
            piece = mixed_ref[i].astype(jnp.float32)
            square = square + jnp.sum(piece * piece, axis=1, keepdims=True)
        scale = lax.rsqrt(square / model_width + EPSILON)
        square = jnp.zeros((tokens, 1), jnp.float32)
        for i in range(pieces):
            cols = pl.ds(i * width, width)
            piece = mixed_ref[i].astype(jnp.float32)
            updated = (
                residual_ref[:, cols].astype(jnp.float32) + piece * scale * mix_gain_ref[:, cols]
            ).astype(jnp.bfloat16)
            updated_ref[:, cols] = updated
            updated = updated.astype(jnp.float32)
            square = square + jnp.sum(updated * updated, axis=1, keepdims=True)
        scale = lax.rsqrt(square / model_width + EPSILON)
        for i in range(pieces):
            cols = pl.ds(i * width, width)
            updated = updated_ref[:, cols].astype(jnp.float32)
            normed_ref[i] = (updated * scale * ffn_gain_ref[:, cols]).astype(jnp.bfloat16)

    for i, out_ref in enumerate(out_refs):
        rows = out_ref.shape[0]
        place = lax.broadcasted_iota(jnp.int32, (rows, tokens), 0) + i * rows
        chosen = (place == slot_ref[0:1, :]) | (place == slot_ref[1:2, :])
        pick = jnp.where(chosen, 1.0, 0.0).astype(jnp.bfloat16)
        out_ref[...] = jnp.dot(
            pick, normed_ref[step], preferred_element_type=jnp.float32
        ).astype(jnp.bfloat16)


def norm_and_spread(mixed, residual, mix_gain, ffn_gain, slot_rows, rows, chunks):
    pieces, tokens, width = mixed.shape
    model_width = pieces * width
    whole = pl.BlockSpec((tokens, model_width), lambda i: (0, 0))
    gain = pl.BlockSpec((1, model_width), lambda i: (0, 0))
    return pl.pallas_call(
        norm_kernel,
        grid=(pieces,),
        in_specs=[
            pl.BlockSpec((pieces, tokens, width), lambda i: (0, 0, 0)),
            whole,
            gain,
            gain,
            pl.BlockSpec((2, tokens), lambda i: (0, 0)),
        ],
        out_specs=[whole] + [pl.BlockSpec((rows, width), lambda i: (0, i))] * chunks,
        out_shape=[
            jax.ShapeDtypeStruct((tokens, model_width), jnp.bfloat16),
        ]
        + [jax.ShapeDtypeStruct((rows, model_width), jnp.bfloat16)] * chunks,
        scratch_shapes=[pltpu.VMEM((pieces, tokens, width), jnp.bfloat16)],
        name="norm_spread",
    )(mixed, residual, mix_gain[None], ffn_gain[None], slot_rows)


def combine_kernel(*refs):
    *back_refs, updated_ref, slot_ref, weight_ref, out_ref = refs
    tokens = updated_ref.shape[0]
    rows = back_refs[0].shape[0]
    slots = rows * len(back_refs)
    place = lax.broadcasted_iota(jnp.int32, (tokens, slots), 1)
    picks = [jnp.where(place == slot_ref[:, k : k + 1], 1.0, 0.0) for k in range(2)]
    pick = jnp.concatenate(picks, axis=0).astype(jnp.bfloat16)
    back = jnp.concatenate([ref[...] for ref in back_refs], axis=0)
    chosen = jnp.dot(pick, back, preferred_element_type=jnp.float32)
    total = updated_ref[...].astype(jnp.float32)
    for k in range(2):
        total += weight_ref[:, k : k + 1] * chosen[k * tokens : (k + 1) * tokens]
    out_ref[...] = total.astype(jnp.bfloat16)


def expert_kernel(*refs, count, pieces):
    row_refs = refs[:count]
    gate_ref, up_ref, down_ref = refs[count : count + 3]
    out_refs = refs[count + 3 : 2 * count + 3]
    gate_sum, up_sum, hidden_ref = refs[2 * count + 3 :]
    rows = row_refs[0].shape[0]
    step = pl.program_id(0)

    @pl.when(step < pieces)
    def _():
        row_block = jnp.concatenate([ref[...] for ref in row_refs], axis=0)
        last = (((1,), (1,)), ((), ()))
        gate = lax.dot_general(row_block, gate_ref[0], last, preferred_element_type=jnp.float32)
        up = lax.dot_general(row_block, up_ref[0], last, preferred_element_type=jnp.float32)

        @pl.when(step == 0)
        def _():
            gate_sum[...] = gate
            up_sum[...] = up

        @pl.when(step > 0)
        def _():
            gate_sum[...] += gate
            up_sum[...] += up

    @pl.when(step == pieces - 1)
    def _():
        hidden_ref[...] = (jax.nn.silu(gate_sum[...]) * up_sum[...]).astype(jnp.bfloat16)

    @pl.when(step >= pieces)
    def _():
        result = jnp.dot(hidden_ref[...], down_ref[0], preferred_element_type=jnp.float32)
        for i, ref in enumerate(out_refs):
            ref[...] = result[i * rows : (i + 1) * rows].astype(jnp.bfloat16)


def run_expert(blocks, gate, up, down, pieces):
    count = len(blocks)
    rows, model_width = blocks[0].shape
    hidden = gate.shape[2]
    width = model_width // pieces

    def first(i):
        return jnp.minimum(i, pieces - 1)

    def second(i):
        return jnp.maximum(i - pieces, 0)

    total = count * rows
    return pl.pallas_call(
        functools.partial(expert_kernel, count=count, pieces=pieces),
        grid=(2 * pieces,),
        in_specs=[pl.BlockSpec((rows, width), lambda i: (0, first(i)))] * count
        + [pl.BlockSpec((1, hidden, width), lambda i: (0, 0, first(i)))] * 2
        + [pl.BlockSpec((1, hidden, width), lambda i: (0, 0, second(i)))],
        out_specs=[pl.BlockSpec((rows, width), lambda i: (0, second(i)))] * count,
        out_shape=[jax.ShapeDtypeStruct((rows, model_width), jnp.bfloat16)] * count,
        scratch_shapes=[
            pltpu.VMEM((total, hidden), jnp.float32),
            pltpu.VMEM((total, hidden), jnp.float32),
            pltpu.VMEM((total, hidden), jnp.bfloat16),
        ],
        cost_estimate=pl.CostEstimate(
            flops=6 * total * model_width * hidden,
            bytes_accessed=6 * model_width * hidden,
            transcendentals=total * hidden,
        ),
        name="expert",
    )(*blocks, jnp.swapaxes(gate, 1, 2), jnp.swapaxes(up, 1, 2), down)


def combine(backs, updated, slot_index, route_weight, pieces):
    rows, model_width = backs[0].shape
    tokens = updated.shape[0]
    width = model_width // pieces
    pair = pl.BlockSpec((tokens, 2), lambda i: (0, 0))
    column = pl.BlockSpec((tokens, width), lambda i: (0, i))
    return pl.pallas_call(
        combine_kernel,
        grid=(pieces,),
        in_specs=[pl.BlockSpec((rows, width), lambda i: (0, i))] * len(backs)
        + [column, pair, pair],
        out_specs=column,
        out_shape=jax.ShapeDtypeStruct((tokens, model_width), jnp.bfloat16),
        name="combine",
    )(*backs, updated, slot_index, route_weight)


def shards(
    queries,
    key_vectors,
    value_vectors,
    residual_in,
    input_logit,
    forget_logit,
    mix_gain,
    ffn_gain,
    expert_gate,
    expert_up,
    expert_down,
    routes,
    route_weight,
):
    tokens, model_width = queries.shape
    head_count = input_logit.shape[0]
    head_dim = model_width // head_count
    devices = lax.axis_size("seq")

    def exchange(array):
        return lax.all_to_all(array, "seq", split_axis=0, concat_axis=0, tiled=True)

    capacity = 4 * tokens // devices
    me = lax.axis_index("seq").astype(jnp.int32)
    flat_routes = routes.reshape(-1)
    matches = (flat_routes[:, None] == jnp.arange(devices, dtype=jnp.int32)[None, :]).astype(
        jnp.int32
    )
    before = jnp.cumsum(matches, axis=0) - matches
    position = jnp.sum(before * matches, axis=1)
    slot_index = ((flat_routes ^ me) * capacity + position).reshape(tokens, 2)

    def trade(array, offset):
        if offset == 0:
            return array
        return lax.ppermute(array, "seq", [(i, i ^ offset) for i in range(devices)])

    packed = exchange(
        pack(queries, key_vectors, value_vectors, input_logit, forget_logit, devices)
    )
    mixed = exchange(mix(packed, tokens, head_dim))
    updated, *spread = norm_and_spread(
        mixed, residual_in, mix_gain, ffn_gain, jnp.transpose(slot_index), capacity, devices
    )
    quarter = devices // 4
    near = list(range(quarter)) + list(range(3 * quarter, devices))
    far = list(range(quarter, 3 * quarter))
    arrived = {k: trade(spread[k], k) for k in near + far}
    returned = {}
    for wave in (near, far):
        results = run_expert(
            [arrived[k] for k in wave], expert_gate, expert_up, expert_down, head_count
        )
        for k, result in zip(wave, results):
            returned[k] = trade(result, k)
    backs = [returned[k] for k in range(devices)]
    return combine(backs, updated, slot_index, route_weight, head_count)


def solution(mesh):
    return jax.shard_map(
        shards,
        mesh=mesh,
        in_specs=(
            P(("batch", "seq"), None),
            P(("batch", "seq"), None),
            P(("batch", "seq"), None),
            P(("batch", "seq"), None),
            P(None, ("batch", "seq")),
            P(None, ("batch", "seq")),
            P(),
            P(),
            P("seq", None, None),
            P("seq", None, None),
            P("seq", None, None),
            P(("batch", "seq"), None),
            P(("batch", "seq"), None),
        ),
        out_specs=P(("batch", "seq"), None),
        check_vma=False,
    )
```
